32 devices in a mesh: grp: 2 (over x), band: 16 (over z, y, core).
Axes of the slice: x: 2, y: 2, z: 4, core: 2. Of those that a mesh axis runs over, the one named last changes fastest.
Arguments:
- source: bfloat16 [262144, 640], P(('grp', 'band')), parts along dimension 0, may hold values from -96 to 96
- tiles: bfloat16 [4096, 128, 128], P('band'), may hold values from 0 to 0.001953125
- tile_slot: int32 [4096], P('band'), may hold values from 0 to 31, as said below
- tile_dst: int32 [4096], P('band'), may hold values from 0 to 31
- send_index: int32 [16, 32], P('band'), may hold values from 0 to 63
- send_count: int32 [16, 16], P('band'), may hold values from 1 to 2, as said below
- polar_tiles: bfloat16 [1024, 128, 128], P('band'), may hold values from 0 to 0.00024414062
- polar_src: int32 [1024], P('band'), may hold values from 0 to 63
- polar_dst: int32 [1024], P('band'), may hold values from 0 to 15
Outputs:
- model_field: bfloat16 [131072, 640], P(('grp', 'band')), parts along dimension 0
- polar_cap: bfloat16 [4096, 640], P(('grp', 'band')), parts along dimension 0
The draws below stay inside these ranges and needn't reach their ends.
There are 2 independent parts, one for each index of `grp`. The reference program is written for one: setup_inputs(seed, part) draws one part's arguments, and reference() takes and returns one part's arrays. A program takes and returns all parts, laid end to end along the dimension named above; an argument that names none is the same for every part. Nothing has to cross between parts.
Inputs may be any that keep to these rules, and one draw needn't show every extreme that they name: `send_count`: entry [s, o] counts the used slots of band s for owner o; every row has an entry 2, and some owner has 2 from every band. `tile_slot`: tile t names slot s * 2 + j of owner t // 256 with j below send_count[s, t // 256]; every used slot is named by some tile of its owner.
All inputs are finite; a program needn't handle non-finite values.
Results may differ from the reference program's by a relative error of at most 0.001.
Values may be sent and summed in bfloat16 or wider, within the bound.
A program may use at most 192 MiB of HBM per device.

```python
import jax
import jax.numpy as jnp
from jax import lax

CH = 80
LEV = 8
BLK = 128
CAP = 2
PB_DEV = 1
SB_DEV = 64
TB_DEV = 32
NT_DEV = 256
PT_DEV = 64
OWNERS = 16
SBLOCKS = 1024
NTILES = 4096
PTILES = 1024
PBLOCKS = 16


def shared_counts(key):
    base = jax.random.fold_in(key, 11)
    first, second, third = jax.random.split(base, 3)
    counts = jax.random.randint(first, (OWNERS, OWNERS), 1, CAP + 1)
    column = jax.random.randint(second, (OWNERS,), 0, OWNERS)
    grid = lax.broadcasted_iota(jnp.int32, (OWNERS, OWNERS), 1)
    counts = jnp.where(grid == column[:, None], CAP, counts)
    busiest = jax.random.randint(third, (), 0, OWNERS)
    counts = jnp.where(grid == busiest, CAP, counts)
    return counts.astype(jnp.int32)


def draw_send_count(key, part):
    return shared_counts(key)


def draw_send_index(key, part):
    base = jax.random.fold_in(key, 13)
    return jax.random.randint(base, (OWNERS, OWNERS * CAP), 0, SB_DEV).astype(jnp.int32)


def draw_tile_slot(key, part):
    counts = shared_counts(key)
    base = jax.random.fold_in(key, 17)
    first, second, third = jax.random.split(base, 3)
    position = lax.broadcasted_iota(jnp.int32, (OWNERS, NT_DEV), 1)
    owner = lax.broadcasted_iota(jnp.int32, (OWNERS, NT_DEV), 0)
    random_sender = jax.random.randint(first, (OWNERS, NT_DEV), 0, OWNERS)
    random_pick = jax.random.randint(second, (OWNERS, NT_DEV), 0, CAP * 64)
    cover = position < OWNERS * CAP
    sender = jnp.where(cover, position // CAP, random_sender)
    pick = jnp.where(cover, position % CAP, random_pick)
    pick = pick % counts[sender, owner]
    slots = sender * CAP + pick
    row_keys = jax.random.split(third, OWNERS)
    orders = jax.vmap(lambda k: jax.random.permutation(k, NT_DEV))(row_keys)
    slots = jnp.take_along_axis(slots, orders, axis=1)
    return slots.reshape(OWNERS * NT_DEV).astype(jnp.int32)


def place_ends(entries, rng, least, high):
    spot = [jax.random.randint(jax.random.fold_in(rng, axis), (), 0, length) for axis, length in enumerate(entries.shape)]
    main_axis = entries.shape.index(max(entries.shape))
    next_to = spot[:main_axis] + [(spot[main_axis] + 1) % entries.shape[main_axis]] + spot[main_axis + 1:]
    return entries.at[tuple(spot)].set(least).at[tuple(next_to)].set(high)


def levels(stream_key, dims, pieces, smallest, high):
    level, own = 1.0, jax.random.fold_in(stream_key, 6)
    for axis_at, parts in pieces:
        heights = jnp.exp(jax.random.uniform(jax.random.fold_in(own, axis_at), (parts,), jnp.float32, smallest / len(pieces), high / len(pieces)))
        level = level * jnp.repeat(heights, dims[axis_at] // parts).reshape([-1 if axis == axis_at else 1 for axis in range(len(dims))])
    return level


def gaussian(own_key, shape, spread, most, pieces=(), kind=jnp.bfloat16):
    array = spread * jax.random.normal(own_key, shape, jnp.float32)
    if pieces:
        array = array * levels(own_key, shape, pieces, -0.22, 0.18)
    return jnp.clip(array, -most, most).astype(kind)


def setup_inputs(seed: int = 0, part: int = 0) -> dict:
    splits = jax.random.split(jax.random.key(seed), 10)
    own_keys = jax.random.split(jax.random.fold_in(splits[9], part), 10)
    source = gaussian(own_keys[0], (SBLOCKS * BLK, LEV * CH), 16.0, 96.0, ((0, 16),))
    tiles = jnp.clip(0.001953125 * jax.random.uniform(splits[1], (NTILES, BLK, BLK), jnp.float32) ** levels(splits[1], (NTILES, BLK, BLK), ((0, 16),), -0.2, 0.2), 0.0, 0.001953125).astype(jnp.bfloat16)
    tile_slot = draw_tile_slot(jax.random.fold_in(splits[9], 71), part)
    tile_dst = place_ends(jax.random.randint(splits[3], (NTILES,), 0, TB_DEV), jax.random.fold_in(splits[3], 1), 0, TB_DEV - 1).astype(jnp.int32)
    send_index = draw_send_index(jax.random.fold_in(splits[9], 71), part)
    send_count = draw_send_count(jax.random.fold_in(splits[9], 71), part)
    polar_tiles = jnp.clip(0.00024414062 * jax.random.uniform(splits[6], (PTILES, BLK, BLK), jnp.float32) ** levels(splits[6], (PTILES, BLK, BLK), ((0, 16),), -0.2, 0.2), 0.0, 0.00024414062).astype(jnp.bfloat16)
    polar_src = place_ends(jax.random.randint(splits[7], (PTILES,), 0, SB_DEV), jax.random.fold_in(splits[7], 1), 0, SB_DEV - 1).astype(jnp.int32)
    polar_dst = place_ends(jax.random.randint(splits[8], (PTILES,), 0, PBLOCKS), jax.random.fold_in(splits[8], 1), 0, PBLOCKS - 1).astype(jnp.int32)
    return dict(source=source, tiles=tiles, tile_slot=tile_slot, tile_dst=tile_dst, send_index=send_index, send_count=send_count, polar_tiles=polar_tiles, polar_src=polar_src, polar_dst=polar_dst)


def reference(source, tiles, tile_slot, tile_dst, send_index, send_count, polar_tiles, polar_src, polar_dst):
    feats = LEV * CH
    blocks = source.reshape(OWNERS * SB_DEV, BLK, feats)

    def owner_field(owner):
        start = owner * NT_DEV
        weights = lax.dynamic_slice_in_dim(tiles, start, NT_DEV, 0).astype(jnp.float32)
        slots = lax.dynamic_slice_in_dim(tile_slot, start, NT_DEV, 0)
        places = lax.dynamic_slice_in_dim(tile_dst, start, NT_DEV, 0)
        sender = slots // CAP
        within = slots % CAP
        local = send_index[sender, owner * CAP + within]
        usable = within < send_count[sender, owner]
        inputs = blocks[(sender * SB_DEV + local).astype(jnp.int32)].astype(jnp.float32)
        inputs = jnp.where(usable[:, None, None], inputs, jnp.zeros((), jnp.float32))
        products = jnp.einsum("tps,tsf->tpf", weights, inputs)
        return jax.ops.segment_sum(products, places, num_segments=TB_DEV)

    field = lax.map(owner_field, jnp.arange(OWNERS, dtype=jnp.int32))
    rounded = field.reshape(OWNERS * TB_DEV, BLK, feats).astype(jnp.bfloat16)
    model_field = rounded.reshape(TB_DEV, OWNERS, BLK, feats).transpose(1, 0, 2, 3).reshape(OWNERS * TB_DEV * BLK, feats)

    def band_cap(total, band):
        start = band * PT_DEV
        weights = lax.dynamic_slice_in_dim(polar_tiles, start, PT_DEV, 0).astype(jnp.float32)
        local = lax.dynamic_slice_in_dim(polar_src, start, PT_DEV, 0)
        places = lax.dynamic_slice_in_dim(polar_dst, start, PT_DEV, 0)
        inputs = blocks[(band * SB_DEV + local).astype(jnp.int32)].astype(jnp.float32)
        products = jnp.einsum("tps,tsf->tpf", weights, inputs)
        return total + jax.ops.segment_sum(products, places, num_segments=PB_DEV * OWNERS), None

    cap_sum, _ = lax.scan(band_cap, jnp.zeros((PB_DEV * OWNERS, BLK, feats), jnp.float32), jnp.arange(OWNERS, dtype=jnp.int32))
    polar_cap = cap_sum.reshape(PB_DEV * OWNERS * BLK, feats).astype(jnp.bfloat16)
    return (model_field, polar_cap)
```

```python
import functools

import jax
import jax.numpy as jnp
from jax import lax
from jax.experimental import pallas as pl
from jax.experimental.pallas import tpu as pltpu
from jax.sharding import PartitionSpec as P

PB_DEV = 1
TB_DEV = 32
GROUP = 4


def plan(dst, slot, blocks):
    count = dst.shape[0]
    groups = count // GROUP + blocks
    same = dst[:, None] == dst[None, :]
    earlier = jnp.arange(count)[:, None] > jnp.arange(count)[None, :]
    rank = jnp.sum(same & earlier, axis=1, dtype=jnp.int32)
    held = jnp.sum(
        dst[None, :] == jnp.arange(blocks, dtype=jnp.int32)[:, None], axis=1, dtype=jnp.int32
    )
    need = (held + GROUP - 1) // GROUP
    ids = jnp.arange(blocks)
    ends = jnp.sum(jnp.where(ids[:, None] >= ids[None, :], need[None, :], 0), axis=1)
    first = ends - need
    start = jnp.sum(
        jnp.where(dst[:, None] == ids[None, :], first[None, :], 0), axis=1, dtype=jnp.int32
    )
    place = start * GROUP + rank
    hit = place[None, :] == jnp.arange(groups * GROUP, dtype=jnp.int32)[:, None]
    tile_at = jnp.sum(
        jnp.where(hit, jnp.arange(1, count + 1, dtype=jnp.int32)[None, :], 0), axis=1
    )
    slot_at = jnp.sum(jnp.where(hit, slot[None, :], 0), axis=1)
    g = jnp.arange(groups, dtype=jnp.int32)
    dst_at = jnp.sum(ends[None, :] <= g[:, None], axis=1, dtype=jnp.int32)
    return tile_at, slot_at, dst_at, ends[-1:]


def block_kernel(tile_at, slot_at, dst_at, total, tiles, inputs, out, acc):
    acc[...] = jnp.zeros_like(acc)

    def step(g, carry):
        weights = []
        values = []
        for i in range(GROUP):
            t = tile_at[g * GROUP + i]
            w = tiles[jnp.maximum(t - 1, 0)]
            weights.append(jnp.where(t > 0, w, jnp.zeros_like(w)))
            values.append(inputs[slot_at[g * GROUP + i]])
        d = dst_at[g]
        acc[d] += jnp.dot(
            jnp.concatenate(weights, axis=1),
            jnp.concatenate(values, axis=0),
            preferred_element_type=jnp.float32,
        )
        return carry

    lax.fori_loop(0, total[0], step, 0)
    if out is not acc:
        out[...] = acc[...].astype(out.dtype)


def cap_kernel(tile_at, slot_at, dst_at, total, tiles, inputs, out):
    block_kernel(tile_at, slot_at, dst_at, total, tiles, inputs, out, out)


def block_matmul(tables, tiles, inputs, blocks, dtype, name):
    count, width, _ = tiles.shape
    feats = inputs.shape[2]
    rounds = dtype != jnp.float32
    return pl.pallas_call(
        block_kernel if rounds else cap_kernel,
        out_shape=jax.ShapeDtypeStruct((blocks, width, feats), dtype),
        in_specs=[pl.BlockSpec(memory_space=pltpu.SMEM)] * 4
        + [pl.BlockSpec(memory_space=pltpu.VMEM)] * 2,
        out_specs=pl.BlockSpec(memory_space=pltpu.VMEM),
        scratch_shapes=[pltpu.VMEM((blocks, width, feats), jnp.float32)] if rounds else [],
        compiler_params=pltpu.CompilerParams(vmem_limit_bytes=56 * 1024 * 1024),
        cost_estimate=pl.CostEstimate(
            flops=4 * count * width * width * feats,
            bytes_accessed=2 * (tiles.size + inputs.size) + 4 * blocks * width * feats,
            transcendentals=0,
        ),
        name=name,
    )(*tables, tiles, inputs)


def gather_kernel(index, blocks, out, held, in_sem, out_sem):
    count = out.shape[0]
    reads = [
        pltpu.make_async_copy(blocks.at[index[0, i]], held.at[i], in_sem.at[i])
        for i in range(count)
    ]
    writes = [
        pltpu.make_async_copy(held.at[i], out.at[i], out_sem.at[i]) for i in range(count)
    ]
    for copy in reads:
        copy.start()
    for read, write in zip(reads, writes):
        read.wait()
        write.start()
    for copy in writes:
        copy.wait()


def gather_blocks(index, blocks):
    count = index.shape[1]
    shape = (count,) + blocks.shape[1:]
    return pl.pallas_call(
        gather_kernel,
        out_shape=jax.ShapeDtypeStruct(shape, blocks.dtype),
        in_specs=[
            pl.BlockSpec(memory_space=pltpu.SMEM),
            pl.BlockSpec(memory_space=pl.ANY),
        ],
        out_specs=pl.BlockSpec(memory_space=pl.ANY),
        scratch_shapes=[
            pltpu.VMEM(shape, blocks.dtype),
            pltpu.SemaphoreType.DMA((count,)),
            pltpu.SemaphoreType.DMA((count,)),
        ],
        name="gather",
    )(index, blocks)


def on_device(
    source, tiles, tile_slot, tile_dst, send_index, send_count, polar_tiles, polar_src, polar_dst
):
    owners = lax.axis_size("band")
    width = tiles.shape[1]
    feats = source.shape[1]
    per_owner = send_index.shape[1] // owners
    blocks = source.reshape(-1, width, feats)
    outgoing = gather_blocks(send_index, blocks)
    received = lax.all_to_all(
        outgoing.reshape(owners, per_owner, width, feats),
        "band",
        split_axis=0,
        concat_axis=0,
        tiled=True,
    )
    arrived = received.reshape(owners * per_owner, width, feats)
    caps = PB_DEV * owners
    cap_part = block_matmul(
        plan(polar_dst, polar_src, caps), polar_tiles, blocks, caps, jnp.float32, "cap"
    )
    own_cap = lax.psum_scatter(cap_part, "band", scatter_dimension=0, tiled=True)
    polar_cap = own_cap.reshape(PB_DEV * width, feats).astype(jnp.bfloat16)
    rounded = block_matmul(
        plan(tile_dst, tile_slot, TB_DEV), tiles, arrived, TB_DEV, jnp.bfloat16, "field"
    ).reshape(TB_DEV // owners, owners, width, feats)
    placed = lax.all_to_all(rounded, "band", split_axis=1, concat_axis=0, tiled=True)
    model_field = placed.reshape(TB_DEV * width, feats)
    return (model_field, polar_cap)


def solution(mesh):
    placed = (
        P(("grp", "band"), None),
        P("band", None, None),
        P("band"),
        P("band"),
        P("band", None),
        P("band", None),
        P("band", None, None),
        P("band"),
        P("band"),
    )
    return jax.shard_map(
        on_device,
        mesh=mesh,
        in_specs=placed,
        out_specs=(P(("grp", "band"), None), P(("grp", "band"), None)),
        check_vma=False,
    )
```

```python
import functools

import jax
import jax.numpy as jnp
from jax import lax
from jax.experimental import pallas as pl
from jax.experimental.pallas import tpu as pltpu
from jax.sharding import PartitionSpec as P

PB_DEV = 1
TB_DEV = 32
GROUP = 4


def plan(dst, slot, blocks):
    count = dst.shape[0]
    groups = count // GROUP + blocks
    same = dst[:, None] == dst[None, :]
    earlier = jnp.arange(count)[:, None] > jnp.arange(count)[None, :]
    rank = jnp.sum(same & earlier, axis=1, dtype=jnp.int32)
    held = jnp.sum(
        dst[None, :] == jnp.arange(blocks, dtype=jnp.int32)[:, None], axis=1, dtype=jnp.int32
    )
    need = (held + GROUP - 1) // GROUP
    ids = jnp.arange(blocks)
    ends = jnp.sum(jnp.where(ids[:, None] >= ids[None, :], need[None, :], 0), axis=1)
    first = ends - need
    start = jnp.sum(
        jnp.where(dst[:, None] == ids[None, :], first[None, :], 0), axis=1, dtype=jnp.int32
    )
    place = start * GROUP + rank
    hit = place[None, :] == jnp.arange(groups * GROUP, dtype=jnp.int32)[:, None]
    tile_at = jnp.sum(
        jnp.where(hit, jnp.arange(1, count + 1, dtype=jnp.int32)[None, :], 0), axis=1
    )
    slot_at = jnp.sum(jnp.where(hit, slot[None, :], 0), axis=1)
    g = jnp.arange(groups, dtype=jnp.int32)
    dst_at = jnp.sum(ends[None, :] <= g[:, None], axis=1, dtype=jnp.int32)
    return tile_at, slot_at, dst_at, ends[-1:]


def block_kernel(tile_at, slot_at, dst_at, total, tiles, inputs, out, acc):
    acc[...] = jnp.zeros_like(acc)

    def step(g, carry):
        weights = []
        values = []
        for i in range(GROUP):
            t = tile_at[g * GROUP + i]
            w = tiles[jnp.maximum(t - 1, 0)]
            weights.append(jnp.where(t > 0, w, jnp.zeros_like(w)))
            values.append(inputs[slot_at[g * GROUP + i]])
        d = dst_at[g]
        acc[d] += jnp.dot(
            jnp.concatenate(weights, axis=1),
            jnp.concatenate(values, axis=0),
            preferred_element_type=jnp.float32,
        )
        return carry

    lax.fori_loop(0, total[0], step, 0)
    if out is not acc:
        out[...] = acc[...].astype(out.dtype)


def cap_kernel(tile_at, slot_at, dst_at, total, tiles, inputs, out):
    block_kernel(tile_at, slot_at, dst_at, total, tiles, inputs, out, out)


def after_kernel(tile_at, slot_at, dst_at, total, tiles, inputs, before, out, acc):
    block_kernel(tile_at, slot_at, dst_at, total, tiles, inputs, out, acc)


def block_matmul(tables, tiles, inputs, blocks, dtype, name, before=()):
    count, width, _ = tiles.shape
    feats = inputs.shape[2]
    rounds = dtype != jnp.float32
    return pl.pallas_call(
        after_kernel if before else block_kernel if rounds else cap_kernel,
        out_shape=jax.ShapeDtypeStruct((blocks, width, feats), dtype),
        in_specs=[pl.BlockSpec(memory_space=pltpu.SMEM)] * 4
        + [pl.BlockSpec(memory_space=pltpu.VMEM)] * 2
        + [pl.BlockSpec(memory_space=pl.ANY)] * len(before),
        out_specs=pl.BlockSpec(memory_space=pltpu.VMEM),
        scratch_shapes=[pltpu.VMEM((blocks, width, feats), jnp.float32)] if rounds else [],
        compiler_params=pltpu.CompilerParams(vmem_limit_bytes=56 * 1024 * 1024),
        cost_estimate=pl.CostEstimate(
            flops=4 * count * width * width * feats,
            bytes_accessed=2 * (tiles.size + inputs.size) + 4 * blocks * width * feats,
            transcendentals=0,
        ),
        name=name,
    )(*tables, tiles, inputs, *before)


def gather_kernel(cuts, index, blocks, *refs):
    parts = len(cuts)
    outs = refs[:parts]
    held, in_sem, out_sem = refs[parts:]
    count = held.shape[0]
    reads = [
        pltpu.make_async_copy(blocks.at[index[0, i]], held.at[i], in_sem.at[i])
        for i in range(count)
    ]
    for copy in reads:
        copy.start()
    for copy in reads:
        copy.wait()
    writes = []
    for c, (low, high) in enumerate(cuts):
        for i in range(count):
            writes.append(
                pltpu.make_async_copy(
                    held.at[i, :, low:high], outs[c].at[i], out_sem.at[c * count + i]
                )
            )
            writes[-1].start()
    for copy in writes:
        copy.wait()


def gather_blocks(index, blocks, cuts):
    count = index.shape[1]
    width = blocks.shape[1]
    return pl.pallas_call(
        functools.partial(gather_kernel, cuts),
        out_shape=[
            jax.ShapeDtypeStruct((count, width, high - low), blocks.dtype) for low, high in cuts
        ],
        in_specs=[
            pl.BlockSpec(memory_space=pltpu.SMEM),
            pl.BlockSpec(memory_space=pl.ANY),
        ],
        out_specs=[pl.BlockSpec(memory_space=pl.ANY)] * len(cuts),
        scratch_shapes=[
            pltpu.VMEM((count,) + blocks.shape[1:], blocks.dtype),
            pltpu.SemaphoreType.DMA((count,)),
            pltpu.SemaphoreType.DMA((count * len(cuts),)),
        ],
        name="gather",
    )(index, blocks)


def feature_cuts(feats):
    lanes = 128
    half = -(-feats // (2 * lanes)) * lanes
    return ((0, half), (half, feats)) if half < feats else ((0, feats),)


def on_device(
    source, tiles, tile_slot, tile_dst, send_index, send_count, polar_tiles, polar_src, polar_dst
):
    owners = lax.axis_size("band")
    width = tiles.shape[1]
    feats = source.shape[1]
    per_owner = send_index.shape[1] // owners
    blocks = source.reshape(-1, width, feats)
    cuts = feature_cuts(feats)
    received = []
    for low_high, outgoing in zip(cuts, gather_blocks(send_index, blocks, cuts)):
        span = low_high[1] - low_high[0]
        got = lax.all_to_all(
            outgoing.reshape(owners, per_owner, width, span),
            "band",
            split_axis=0,
            concat_axis=0,
            tiled=True,
        )
        received.append(got.reshape(owners * per_owner, width, span))
    caps = PB_DEV * owners
    cap_part = block_matmul(
        plan(polar_dst, polar_src, caps), polar_tiles, blocks, caps, jnp.float32, "cap"
    )
    own_cap = lax.psum_scatter(cap_part, "band", scatter_dimension=0, tiled=True)
    polar_cap = own_cap.reshape(PB_DEV * width, feats).astype(jnp.bfloat16)
    turn = TB_DEV // owners
    target = (tile_dst % owners) * turn + tile_dst // owners
    tables = plan(target, tile_slot, TB_DEV)
    placed = []
    for arrived in received:
        span = arrived.shape[2]
        before = (cap_part,)
        rounded = block_matmul(tables, tiles, arrived, TB_DEV, jnp.bfloat16, "field", before)
        sent = lax.all_to_all(
            rounded.reshape(owners, turn, width, span),
            "band",
            split_axis=0,
            concat_axis=0,
            tiled=True,
        )
        placed.append(sent.reshape(TB_DEV * width, span))
    return (jnp.concatenate(placed, axis=1), polar_cap)


def solution(mesh):
    placed = (
        P(("grp", "band"), None),
        P("band", None, None),
        P("band"),
        P("band"),
        P("band", None),
        P("band", None),
        P("band", None, None),
        P("band"),
        P("band"),
    )
    return jax.shard_map(
        on_device,
        mesh=mesh,
        in_specs=placed,
        out_specs=(P(("grp", "band"), None), P(("grp", "band"), None)),
        check_vma=False,
    )
```

```python
import functools

import jax
import jax.numpy as jnp
from jax import lax
from jax.experimental import pallas as pl
from jax.experimental.pallas import tpu as pltpu
from jax.sharding import PartitionSpec as P

PB_DEV = 1
TB_DEV = 32
GROUP = 4


def plan(dst, slot, blocks):
    count = dst.shape[0]
    groups = count // GROUP + blocks
    same = dst[:, None] == dst[None, :]
    earlier = jnp.arange(count)[:, None] > jnp.arange(count)[None, :]
    rank = jnp.sum(same & earlier, axis=1, dtype=jnp.int32)
    held = jnp.sum(
        dst[None, :] == jnp.arange(blocks, dtype=jnp.int32)[:, None], axis=1, dtype=jnp.int32
    )
    need = (held + GROUP - 1) // GROUP
    ids = jnp.arange(blocks)
    ends = jnp.sum(jnp.where(ids[:, None] >= ids[None, :], need[None, :], 0), axis=1)
    first = ends - need
    start = jnp.sum(
        jnp.where(dst[:, None] == ids[None, :], first[None, :], 0), axis=1, dtype=jnp.int32
    )
    place = start * GROUP + rank
    hit = place[None, :] == jnp.arange(groups * GROUP, dtype=jnp.int32)[:, None]
    tile_at = jnp.sum(
        jnp.where(hit, jnp.arange(1, count + 1, dtype=jnp.int32)[None, :], 0), axis=1
    )
    slot_at = jnp.sum(jnp.where(hit, slot[None, :], 0), axis=1)
    g = jnp.arange(groups, dtype=jnp.int32)
    dst_at = jnp.sum(ends[None, :] <= g[:, None], axis=1, dtype=jnp.int32)
    return tile_at, slot_at, dst_at, ends[-1:]


def block_kernel(tile_at, slot_at, dst_at, total, tiles, inputs, out, acc):
    acc[...] = jnp.zeros_like(acc)

    def step(g, carry):
        weights = []
        values = []
        for i in range(GROUP):
            t = tile_at[g * GROUP + i]
            w = tiles[jnp.maximum(t - 1, 0)]
            weights.append(jnp.where(t > 0, w, jnp.zeros_like(w)))
            values.append(inputs[slot_at[g * GROUP + i]])
        d = dst_at[g]
        acc[d] += jnp.dot(
            jnp.concatenate(weights, axis=1),
            jnp.concatenate(values, axis=0),
            preferred_element_type=jnp.float32,
        )
        return carry

    lax.fori_loop(0, total[0], step, 0)
    if out is not acc:
        out[...] = acc[...].astype(out.dtype)


def cap_kernel(tile_at, slot_at, dst_at, total, tiles, inputs, before, out):
    block_kernel(tile_at, slot_at, dst_at, total, tiles, inputs, out, out)


def after_kernel(tile_at, slot_at, dst_at, total, tiles, inputs, before, out, acc):
    block_kernel(tile_at, slot_at, dst_at, total, tiles, inputs, out, acc)


def block_matmul(tables, tiles, inputs, blocks, dtype, name, before=()):
    count, width, _ = tiles.shape
    feats = inputs.shape[2]
    rounds = dtype != jnp.float32
    return pl.pallas_call(
        after_kernel if rounds else cap_kernel,
        out_shape=jax.ShapeDtypeStruct((blocks, width, feats), dtype),
        in_specs=[pl.BlockSpec(memory_space=pltpu.SMEM)] * 4
        + [pl.BlockSpec(memory_space=pltpu.VMEM)] * 2
        + [pl.BlockSpec(memory_space=pl.ANY)] * len(before),
        out_specs=pl.BlockSpec(memory_space=pltpu.VMEM),
        scratch_shapes=[pltpu.VMEM((blocks, width, feats), jnp.float32)] if rounds else [],
        compiler_params=pltpu.CompilerParams(vmem_limit_bytes=56 * 1024 * 1024),
        cost_estimate=pl.CostEstimate(
            flops=4 * count * width * width * feats,
            bytes_accessed=2 * (tiles.size + inputs.size) + 4 * blocks * width * feats,
            transcendentals=0,
        ),
        name=name,
    )(*tables, tiles, inputs, *before)


def gather_kernel(cuts, index, blocks, *refs):
    parts = len(cuts)
    outs = refs[:parts]
    held, in_sem, out_sem = refs[parts:]
    count = held.shape[0]
    reads = [
        pltpu.make_async_copy(blocks.at[index[0, i]], held.at[i], in_sem.at[i])
        for i in range(count)
    ]
    for copy in reads:
        copy.start()
    for copy in reads:
        copy.wait()
    writes = []
    for c, (low, high) in enumerate(cuts):
        for i in range(count):
            writes.append(
                pltpu.make_async_copy(
                    held.at[i, :, low:high], outs[c].at[i], out_sem.at[c * count + i]
                )
            )
            writes[-1].start()
    for copy in writes:
        copy.wait()


def gather_blocks(index, blocks, cuts):
    count = index.shape[1]
    width = blocks.shape[1]
    return pl.pallas_call(
        functools.partial(gather_kernel, cuts),
        out_shape=[
            jax.ShapeDtypeStruct((count, width, high - low), blocks.dtype) for low, high in cuts
        ],
        in_specs=[
            pl.BlockSpec(memory_space=pltpu.SMEM),
            pl.BlockSpec(memory_space=pl.ANY),
        ],
        out_specs=[pl.BlockSpec(memory_space=pl.ANY)] * len(cuts),
        scratch_shapes=[
            pltpu.VMEM((count,) + blocks.shape[1:], blocks.dtype),
            pltpu.SemaphoreType.DMA((count,)),
            pltpu.SemaphoreType.DMA((count * len(cuts),)),
        ],
        name="gather",
    )(index, blocks)


def feature_cuts(feats):
    lanes = 128
    half = -(-feats // (2 * lanes)) * lanes
    return ((0, half), (half, feats)) if half < feats else ((0, feats),)


def halve(parts, stride):
    owners = lax.axis_size("band")
    bit = lax.rem(lax.axis_index("band") // stride, 2)
    pairs = parts.reshape((-1, 2) + parts.shape[1:])
    keep = lax.dynamic_index_in_dim(pairs, bit, 1, keepdims=False)
    send = lax.dynamic_index_in_dim(pairs, 1 - bit, 1, keepdims=False)
    got = lax.ppermute(send, "band", [(i, i ^ stride) for i in range(owners)])
    return keep + got


def reduce_caps(parts):
    owners = lax.axis_size("band")
    stride = 1
    while stride < 4 and owners % (2 * stride) == 0:
        parts = halve(parts, stride)
        stride *= 2
    groups = [list(range(i, owners, stride)) for i in range(stride)]
    got = lax.all_to_all(
        parts, "band", split_axis=0, concat_axis=0, axis_index_groups=groups, tiled=True
    )
    return jnp.sum(got, axis=0)


def on_device(
    source, tiles, tile_slot, tile_dst, send_index, send_count, polar_tiles, polar_src, polar_dst
):
    owners = lax.axis_size("band")
    width = tiles.shape[1]
    feats = source.shape[1]
    per_owner = send_index.shape[1] // owners
    blocks = source.reshape(-1, width, feats)
    cuts = feature_cuts(feats)
    received = []
    gathered = gather_blocks(send_index, blocks, cuts)
    for low_high, outgoing in zip(cuts, gathered):
        span = low_high[1] - low_high[0]
        got = lax.all_to_all(
            outgoing.reshape(owners, per_owner, width, span),
            "band",
            split_axis=0,
            concat_axis=0,
            tiled=True,
        )
        received.append(got.reshape(owners * per_owner, width, span))
    caps = PB_DEV * owners
    cap_part = block_matmul(
        plan(polar_dst, polar_src, caps), polar_tiles, blocks, caps, jnp.float32, "cap", gathered[:1]
    )
    own_cap = reduce_caps(cap_part.reshape(owners, PB_DEV * width, feats))
    polar_cap = own_cap.reshape(PB_DEV * width, feats).astype(jnp.bfloat16)
    turn = TB_DEV // owners
    target = (tile_dst % owners) * turn + tile_dst // owners
    tables = plan(target, tile_slot, TB_DEV)
    placed = []
    for arrived in received:
        span = arrived.shape[2]
        before = (cap_part,)
        rounded = block_matmul(tables, tiles, arrived, TB_DEV, jnp.bfloat16, "field", before)
        sent = lax.all_to_all(
            rounded.reshape(owners, turn, width, span),
            "band",
            split_axis=0,
            concat_axis=0,
            tiled=True,
        )
        placed.append(sent.reshape(TB_DEV * width, span))
    return (jnp.concatenate(placed, axis=1), polar_cap)


def solution(mesh):
    placed = (
        P(("grp", "band"), None),
        P("band", None, None),
        P("band"),
        P("band"),
        P("band", None),
        P("band", None),
        P("band", None, None),
        P("band"),
        P("band"),
    )
    return jax.shard_map(
        on_device,
        mesh=mesh,
        in_specs=placed,
        out_specs=(P(("grp", "band"), None), P(("grp", "band"), None)),
        check_vma=False,
    )
```
